256 devices in a mesh: snap: 4 (over z_hi), param: 64 (over z_lo, x, y, core).
Axes of the slice: x: 4, y: 4, z: 8 (z_hi: 4, z_lo: 2; z = z_hi * 2 + z_lo), core: 2. Of those that a mesh axis runs over, the one named last changes fastest.
Arguments:
- snapshots: bfloat16 [256, 4096, 1024], P('snap', 'param'), as said below
- coeffs: float32 [16, 256], P(None, 'snap'), may hold values from -0.375 to 0.375
Outputs:
- averages: float32 [16, 4096, 1024], P(None, 'param', 'snap')
- width_norms: float32 [16], replicated
The draws below stay inside these ranges and needn't reach their ends.
Inputs may be any that keep to these rules, and one draw needn't show every extreme that they name: `snapshots`: stored snapshot weights, finite.
All inputs are finite; a program needn't handle non-finite values.
Results may differ from the reference program's by a relative error of at most 0.0003.
Values may be sent and summed in bfloat16 or wider, within the bound.
A program may use at most 64 MiB of HBM per device.

```python
import math
import jax
import jax.numpy as jnp
from jax import lax

WIDTHS = 16
COLS = 1024
NSNAP = 256
ROWS = 4096


def draw_snapshots(key, part):
    key_rows = jax.random.fold_in(key, 11)
    key_cols = jax.random.fold_in(key, 12)
    key_base = jax.random.fold_in(key, 13)
    row_index = jnp.arange(ROWS, dtype=jnp.float32)
    row_scale = 3.0 ** (row_index / ROWS) * 10.0 ** jax.random.uniform(key_rows, (ROWS,), jnp.float32)
    col_scale = 10.0 ** jax.random.uniform(key_cols, (COLS,), jnp.float32)
    base = jax.random.normal(key_base, (NSNAP, ROWS, COLS), jnp.float32)
    values = base * row_scale[None, :, None] * col_scale[None, None, :] / 10.0
    return values.astype(jnp.bfloat16)


def block_scale(key, shape, shards, least, largest):
    loudness, own = 1.0, jax.random.fold_in(key, 6)
    for dim, blocks in shards:
        draws = jnp.exp(jax.random.uniform(jax.random.fold_in(own, dim), (blocks,), jnp.float32, least / len(shards), largest / len(shards)))
        loudness = loudness * jnp.repeat(draws, shape[dim] // blocks).reshape([-1 if axis == dim else 1 for axis in range(len(shape))])
    return loudness


def gaussian(rng, extent, deviation, most, cuts=(), kind=jnp.bfloat16):
    values = jax.random.normal(rng, extent, jnp.float32) * deviation
    if len(cuts) > 0:
        values = block_scale(rng, extent, cuts, -0.22, 0.18) * values
    return jnp.clip(values, min=-most, max=most).astype(kind)


def setup_inputs(seed: int = 0) -> dict:
    splits = jax.random.split(jax.random.key(seed), 3)
    snapshots = draw_snapshots(jax.random.fold_in(splits[2], 71), 0)
    coeffs = gaussian(splits[1], (WIDTHS, NSNAP), NSNAP ** -0.5, 0.375, ((1, 4),), jnp.float32)
    return dict(snapshots=snapshots, coeffs=coeffs)


def reference(snapshots, coeffs):
    block_rows = math.gcd(ROWS, 256)
    block_count = ROWS // block_rows

    def one_block(block_index):
        start = (block_index * block_rows).astype(jnp.int32)
        piece = lax.dynamic_slice_in_dim(snapshots, start, block_rows, 1).astype(jnp.float32)
        flat = piece.reshape(NSNAP, block_rows * COLS)
        product = jnp.dot(coeffs.astype(jnp.float32), flat, precision=lax.Precision.HIGHEST, preferred_element_type=jnp.float32)
        return product.reshape(WIDTHS, block_rows, COLS)
    stacked = lax.map(one_block, jnp.arange(block_count, dtype=jnp.int32))
    averages = jnp.transpose(stacked, (1, 0, 2, 3)).reshape(WIDTHS, ROWS, COLS)
    squares = lax.optimization_barrier(jnp.sum(averages * averages, axis=(1, 2)))
    width_norms = jnp.sqrt(squares / jnp.float32(ROWS * COLS))
    return (averages, width_norms)
```

```python
import functools

import jax
import jax.numpy as jnp
from jax import lax
from jax.experimental import pallas as pl
from jax.experimental.pallas import tpu as pltpu
from jax.sharding import Mesh
from jax.sharding import PartitionSpec as P

MESH = pl.DeviceIdType.MESH
PARAM = ("zlo", "x", "y", "core")
ROWS = 16
LEAST = -125.0
SPAN = 251.5
TINY = 1e-37


def encode(value):
    size = jnp.abs(value)
    largest = jnp.max(jnp.max(size, axis=0), axis=0, keepdims=True)
    largest = jnp.maximum(largest, TINY)
    inverse = 1.0 / largest
    power = jnp.exp2((size * inverse[None]) * SPAN + LEAST)
    return jnp.where(value < 0, -power, power).astype(jnp.bfloat16), largest


def decode(codes, largest):
    code = codes.astype(jnp.float32)
    size = (jnp.log2(jnp.abs(code)) - LEAST) * (largest * (1.0 / SPAN))[None]
    return jnp.where(code < 0, -size, size)


def tile_of(i):
    return (i % 2) * 2 + i // 2, 2 * (i % 2) - 1


def kernel(sizes, coeffs_hbm, snap_hbm, avg_hbm, norm_ref,
           coef, stage, kron, share, sent, sent_max, got, got_max, total, squares,
           note, seen1, seen2,
           coef_sem, stage_sem, out_sem, send_sem, send_max_sem, recv_sem, recv_max_sem,
           note1_send, note1_recv, note2_send, note2_recv):
    widths, snaps, cols, entries = sizes
    q = lax.axis_index("snap")
    zlo, x, y, core = (lax.axis_index(a) for a in PARAM)
    line = (q * 2 + zlo) * 2 + core
    plane = x * 4 + y

    def line_peer(k):
        p = (line + k) % 16
        return p, {"snap": p // 4, "zlo": (p // 2) % 2, "core": p % 2}

    def plane_peer(k):
        p = (plane + k) % 16
        return p, {"x": p // 4, "y": p % 4}

    barrier = pltpu.get_barrier_semaphore()

    def load(k):
        kind, i = k // 4, k % 4
        tile, way = tile_of(i)
        block = (q + jnp.where(kind == 0, 2, jnp.where(kind == 1, 4 - way, jnp.where(kind == 2, 4 + way, 0)))) % 4
        return pltpu.make_async_copy(
            snap_hbm.at[:, pl.ds(pl.multiple_of(tile * ROWS, ROWS), ROWS),
                        pl.ds(pl.multiple_of(block * cols, cols), cols)],
            stage.at[k], stage_sem.at[k])

    load(0).start()
    coef_copy = pltpu.make_async_copy(coeffs_hbm, coef, coef_sem)
    coef_copy.start()
    for k in range(1, 16):
        _, peer = line_peer(k)
        pl.semaphore_signal(barrier, inc=1, device_id=peer, device_id_type=MESH)
        _, peer = plane_peer(k)
        pl.semaphore_signal(barrier, inc=1, device_id=peer, device_id_type=MESH)
    for k in range(1, 16):
        load(k).start()

    coef_copy.wait()
    part = coef[...]
    m, n = widths * ROWS, snaps * ROWS
    up = jnp.where(lax.broadcasted_iota(jnp.int32, (m, widths), 0) // ROWS
                   == lax.broadcasted_iota(jnp.int32, (m, widths), 1), 1.0, 0.0).astype(jnp.bfloat16)
    across = jnp.where(lax.broadcasted_iota(jnp.int32, (snaps, n), 1) // ROWS
                       == lax.broadcasted_iota(jnp.int32, (snaps, n), 0), 1.0, 0.0).astype(jnp.bfloat16)
    same = (lax.broadcasted_iota(jnp.int32, (m, n), 0) % ROWS
            == lax.broadcasted_iota(jnp.int32, (m, n), 1) % ROWS)
    for half in range(2):
        top = part.astype(jnp.bfloat16)
        part = part - top.astype(jnp.float32)
        spread = jnp.dot(up, top, preferred_element_type=jnp.float32).astype(jnp.bfloat16)
        spread = jnp.dot(spread, across, preferred_element_type=jnp.float32)
        kron[pl.ds(half * m, m), :] = jnp.where(same, spread, 0.0).astype(jnp.bfloat16)

    def product(k):
        load(k).wait()
        both = jnp.dot(kron[...], stage[k].reshape(n, cols), preferred_element_type=jnp.float32)
        return (both[:m] + both[m:]).reshape(widths, ROWS, cols)

    def copies(k, target):
        peer = {"snap": (q + target + 4) % 4}
        return (
            pltpu.make_async_remote_copy(
                src_ref=sent_max.at[k], dst_ref=got_max.at[k], send_sem=send_max_sem.at[k],
                recv_sem=recv_max_sem.at[k], device_id=peer, device_id_type=MESH),
            pltpu.make_async_remote_copy(
                src_ref=sent.at[k], dst_ref=got.at[k], send_sem=send_sem.at[k],
                recv_sem=recv_sem.at[k], device_id=peer, device_id_type=MESH),
        )

    def put(k, value):
        sent[k], sent_max[k] = encode(value)

    def send(k, target):
        for copy in copies(k, target):
            copy.start()

    def receive(k):
        for copy in copies(k, 1):
            copy.wait_recv()
        return decode(got[k], got_max[k])

    put(0, product(0))
    pl.semaphore_wait(barrier, 30)
    send(0, -1)

    def first(k, _):
        tile, way = tile_of(k % 4)
        put(k, product(k))
        send(k, jnp.where(k < 4, way, -way))
        return 0

    lax.fori_loop(1, 8, first, 0)

    def mine(i, _):
        total[i] = product(12 + i)
        return 0

    lax.fori_loop(0, 4, mine, 0)

    def forward(i, _):
        tile, way = tile_of(i)
        put(8 + i, product(8 + i) + receive(i))
        send(8 + i, way)
        return 0

    lax.fori_loop(0, 4, forward, 0)

    def direct(i, _):
        total[i] = total[i] + receive(4 + i)
        return 0

    lax.fori_loop(0, 4, direct, 0)
    squares[...] = jnp.zeros_like(squares)

    def out(i):
        tile, way = tile_of(i)
        return pltpu.make_async_copy(
            total.at[i], avg_hbm.at[:, pl.ds(pl.multiple_of(tile * ROWS, ROWS), ROWS), :], out_sem.at[i])

    def last(i, _):
        value = total[i] + receive(8 + i)
        total[i] = value
        out(i).start()
        squares[...] += jnp.sum(value * value, axis=1)
        return 0

    lax.fori_loop(0, 4, last, 0)

    per = jnp.sum(squares[...], axis=1, keepdims=True)
    spot = (lax.broadcasted_iota(jnp.int32, (widths, 128), 0)
            == lax.broadcasted_iota(jnp.int32, (widths, 128), 1))
    value = jnp.sum(jnp.where(spot, per, 0.0), axis=0, keepdims=True)
    for step, (here, peer_of, seen, ssem, rsem) in enumerate((
            (line, line_peer, seen1, note1_send, note1_recv),
            (plane, plane_peer, seen2, note2_send, note2_recv))):
        note[step] = value
        seen[here] = value

        def message(k):
            p, peer = peer_of(k)
            return p, pltpu.make_async_remote_copy(
                src_ref=note.at[step], dst_ref=seen.at[here], send_sem=ssem.at[k - 1],
                recv_sem=rsem.at[here], device_id=peer, device_id_type=MESH)

        for k in range(1, 16):
            message(k)[1].start()
        for k in range(1, 16):
            p, _ = peer_of(k)
            pltpu.make_async_remote_copy(
                src_ref=note.at[step], dst_ref=seen.at[p], send_sem=ssem.at[k - 1],
                recv_sem=rsem.at[p], device_id=peer_of(k)[1], device_id_type=MESH).wait_recv()
        value = jnp.sum(seen[...], axis=0)
    norm_ref[...] = jnp.sqrt(value / jnp.float32(entries))

    for step, (peer_of, seen, ssem, rsem, here) in enumerate((
            (line_peer, seen1, note1_send, note1_recv, line),
            (plane_peer, seen2, note2_send, note2_recv, plane))):
        for k in range(1, 16):
            pltpu.make_async_remote_copy(
                src_ref=note.at[step], dst_ref=seen.at[here], send_sem=ssem.at[k - 1],
                recv_sem=rsem.at[here], device_id=peer_of(k)[1], device_id_type=MESH).wait_send()

    def drain(k, _):
        for copy in copies(k, 1):
            copy.wait_send()
        return 0

    lax.fori_loop(0, 12, drain, 0)
    for i in range(4):
        out(i).wait()


def on_device(snapshots, coeffs):
    widths, snaps = coeffs.shape
    _, rows, all_cols = snapshots.shape
    cols = all_cols // 4
    entries = rows * all_cols * 64
    pieces = 16
    averages, norms = pl.pallas_call(
        functools.partial(kernel, (widths, snaps, cols, entries)),
        out_shape=(jax.ShapeDtypeStruct((widths, rows, cols), jnp.float32),
                   jax.ShapeDtypeStruct((1, 128), jnp.float32)),
        in_specs=[pl.BlockSpec(memory_space=pl.ANY)] * 2,
        out_specs=(pl.BlockSpec(memory_space=pl.ANY), pl.BlockSpec(memory_space=pltpu.VMEM)),
        scratch_shapes=[
            pltpu.VMEM((widths, snaps), jnp.float32),
            pltpu.VMEM((pieces, snaps, ROWS, cols), jnp.bfloat16),
            pltpu.VMEM((2 * widths * ROWS, snaps * ROWS), jnp.bfloat16),
            pltpu.VMEM((4, widths, ROWS, cols), jnp.float32),
            pltpu.VMEM((12, widths, ROWS, cols), jnp.bfloat16),
            pltpu.VMEM((12, 1, cols), jnp.float32),
            pltpu.VMEM((12, widths, ROWS, cols), jnp.bfloat16),
            pltpu.VMEM((12, 1, cols), jnp.float32),
            pltpu.VMEM((4, widths, ROWS, cols), jnp.float32),
            pltpu.VMEM((widths, cols), jnp.float32),
            pltpu.VMEM((2, 1, 128), jnp.float32),
            pltpu.VMEM((16, 1, 128), jnp.float32),
            pltpu.VMEM((16, 1, 128), jnp.float32),
            pltpu.SemaphoreType.DMA,
            pltpu.SemaphoreType.DMA((pieces,)),
            pltpu.SemaphoreType.DMA((4,)),
            pltpu.SemaphoreType.DMA((12,)),
            pltpu.SemaphoreType.DMA((12,)),
            pltpu.SemaphoreType.DMA((12,)),
            pltpu.SemaphoreType.DMA((12,)),
            pltpu.SemaphoreType.DMA((15,)),
            pltpu.SemaphoreType.DMA((16,)),
            pltpu.SemaphoreType.DMA((15,)),
            pltpu.SemaphoreType.DMA((16,)),
        ],
        compiler_params=pltpu.CompilerParams(collective_id=0, has_side_effects=True),
    )(coeffs, snapshots)
    return averages, norms[0, :widths]


def solution(mesh):
    split = Mesh(mesh.devices.reshape(mesh.shape["snap"], 2, 4, 4, 2), ("snap",) + PARAM)
    return jax.shard_map(
        on_device,
        mesh=split,
        in_specs=(P("snap", PARAM, None), P(None, "snap")),
        out_specs=(P(None, PARAM, "snap"), P()),
        check_vma=False,
    )
```

```python
import functools

import jax
import jax.numpy as jnp
from jax import lax
from jax.experimental import pallas as pl
from jax.experimental.pallas import tpu as pltpu
from jax.sharding import Mesh
from jax.sharding import PartitionSpec as P

MESH = pl.DeviceIdType.MESH
PARAM = ("zlo", "x", "y", "core")
ROWS = 16
LEAST = -125.0
SPAN = 251.5
TINY = 1e-37


def encode(value):
    size = jnp.abs(value)
    largest = jnp.max(jnp.max(size, axis=0), axis=0, keepdims=True)
    largest = jnp.maximum(largest, TINY)
    inverse = 1.0 / largest
    power = jnp.exp2((size * inverse[None]) * SPAN + LEAST)
    return jnp.where(value < 0, -power, power).astype(jnp.bfloat16), largest


def decode(codes, largest):
    code = codes.astype(jnp.float32)
    size = (jnp.log2(jnp.abs(code)) - LEAST) * (largest * (1.0 / SPAN))[None]
    return jnp.where(code < 0, -size, size)


def tile_of(i):
    return (i % 2) * 2 + i // 2, 2 * (i % 2) - 1


def kernel(sizes, coeffs_hbm, snap_hbm, avg_out, norm_out,
           avg, norm, coef, stage, kron, sent, sent_max, got, got_max, squares,
           note, seen1, seen2,
           coef_sem, stage_sem, out_sem, norm_sem, relay_sem, send_sem, send_max_sem, recv_sem, recv_max_sem,
           note1_send, note1_recv, note2_send, note2_recv):
    widths, snaps, cols, entries = sizes
    q = lax.axis_index("snap")
    zlo, x, y, core = (lax.axis_index(a) for a in PARAM)
    line = (q * 2 + zlo) * 2 + core
    plane = x * 4 + y

    def line_peer(k):
        p = (line + k) % 16
        return p, {"snap": p // 4, "zlo": (p // 2) % 2, "core": p % 2}

    def plane_peer(k):
        p = (plane + k) % 16
        return p, {"x": p // 4, "y": p % 4}

    def line_at(dz, dc):
        z = (q * 2 + zlo + dz + 8) % 8
        return {"snap": z // 2, "zlo": z % 2, "core": (core + dc) % 2}

    def plane_at(dx, dy):
        return {"x": (x + dx + 4) % 4, "y": (y + dy + 4) % 4}

    barrier = pltpu.get_barrier_semaphore()

    def load(k):
        kind, i = k // 4, k % 4
        tile, way = tile_of(i)
        block = (q + jnp.where(kind == 0, 2, jnp.where(kind == 1, 4 - way, jnp.where(kind == 2, 4 + way, 0)))) % 4
        return pltpu.make_async_copy(
            snap_hbm.at[:, pl.ds(pl.multiple_of(tile * ROWS, ROWS), ROWS),
                        pl.ds(pl.multiple_of(block * cols, cols), cols)],
            stage.at[k], stage_sem.at[k])

    coef_copy = pltpu.make_async_copy(coeffs_hbm, coef, coef_sem)
    coef_copy.start()
    load(0).start()
    load(1).start()
    near = [line_at(dz, dc) for dz in (-2, 2, -1, 1, 0) for dc in (0, 1) if dz or dc]
    near += [plane_at(dx, dy) for dx, dy in ((1, 0), (-1, 0), (2, 0), (0, 1), (0, -1), (0, 2),
                                             (1, 1), (1, -1), (-1, 1), (-1, -1))]
    for peer in near:
        pl.semaphore_signal(barrier, inc=1, device_id=peer, device_id_type=MESH)
    for k in range(2, 16):
        load(k).start()

    m, n = widths * ROWS, snaps * ROWS
    across = jnp.where(lax.broadcasted_iota(jnp.int32, (snaps, n), 1) // ROWS
                       == lax.broadcasted_iota(jnp.int32, (snaps, n), 0), 1.0, 0.0).astype(jnp.bfloat16)
    same = (lax.broadcasted_iota(jnp.int32, (m, n), 0) % ROWS
            == lax.broadcasted_iota(jnp.int32, (m, n), 1) % ROWS)
    with jax.named_scope("coef_wait"):
        coef_copy.wait()
    part = jnp.broadcast_to(coef[...][:, None, :], (widths, ROWS, snaps)).reshape(m, snaps)
    for half in range(2):
        top = part.astype(jnp.bfloat16)
        part = part - top.astype(jnp.float32)
        spread = jnp.dot(top, across, preferred_element_type=jnp.float32)
        kron[pl.ds(half * m, m), :] = jnp.where(same, spread, 0.0).astype(jnp.bfloat16)

    def product(k):
        load(k).wait()
        both = jnp.dot(kron[...], stage[k].reshape(n, cols), preferred_element_type=jnp.float32)
        return (both[:m] + both[m:]).reshape(widths, ROWS, cols)

    def copies(k, target):
        peer = {"snap": (q + target + 4) % 4}
        return (
            pltpu.make_async_remote_copy(
                src_ref=sent_max.at[k], dst_ref=got_max.at[k], send_sem=send_max_sem.at[k],
                recv_sem=recv_max_sem.at[k], device_id=peer, device_id_type=MESH),
            pltpu.make_async_remote_copy(
                src_ref=sent.at[k], dst_ref=got.at[k], send_sem=send_sem.at[k],
                recv_sem=recv_sem.at[k], device_id=peer, device_id_type=MESH),
        )

    def put(k, value):
        sent[k], sent_max[k] = encode(value)

    def send(k, target):
        for copy in copies(k, target):
            copy.start()

    def receive(k):
        for copy in copies(k, 1):
            copy.wait_recv()
        return decode(got[k], got_max[k])

    with jax.named_scope("product0"):
        put(0, product(0))
    with jax.named_scope("barrier"):
        pl.semaphore_wait(barrier, len(near))
    send(0, -1)
    relays = [line_at(-2, 0), line_at(2, 0), plane_at(2, 0), plane_at(0, 2)]
    for peer in relays:
        pl.semaphore_signal(relay_sem, inc=1, device_id=peer, device_id_type=MESH)

    def first(k, _):
        tile, way = tile_of(k % 4)
        put(k, product(k))
        send(k, jnp.where(k < 4, way, -way))
        return 0

    with jax.named_scope("first"):
        lax.fori_loop(1, 8, first, 0)

    def rows_of(i):
        return pl.ds(pl.multiple_of(tile_of(i)[0] * ROWS, ROWS), ROWS)

    def mine(i, _):
        avg[:, rows_of(i), :] = product(12 + i)
        return 0

    with jax.named_scope("mine"):
        lax.fori_loop(0, 4, mine, 0)

    def forward(i, _):
        tile, way = tile_of(i)
        put(8 + i, product(8 + i) + receive(i))
        send(8 + i, way)
        return 0

    with jax.named_scope("forward"):
        lax.fori_loop(0, 4, forward, 0)

    def direct(i, _):
        avg[:, rows_of(i), :] += receive(4 + i)
        return 0

    with jax.named_scope("direct"):
        lax.fori_loop(0, 4, direct, 0)
    squares[...] = jnp.zeros_like(squares)
    with jax.named_scope("relay"):
        pl.semaphore_wait(relay_sem, len(relays))

    def last(i, _):
        value = avg[:, rows_of(i), :] + receive(8 + i)
        avg[:, rows_of(i), :] = value
        squares[...] += jnp.sum(value * value, axis=1)
        return 0

    with jax.named_scope("last"):
        lax.fori_loop(0, 4, last, 0)

    out = pltpu.make_async_copy(avg, avg_out, out_sem)
    out.start()

    per = jnp.sum(squares[...], axis=1, keepdims=True)
    spot = (lax.broadcasted_iota(jnp.int32, (widths, 128), 0)
            == lax.broadcasted_iota(jnp.int32, (widths, 128), 1))
    value = jnp.sum(jnp.where(spot, per, 0.0), axis=0, keepdims=True)
    for step, (here, peer_of, seen, ssem, rsem) in enumerate((
            (line, line_peer, seen1, note1_send, note1_recv),
            (plane, plane_peer, seen2, note2_send, note2_recv))):
        note[step] = value
        seen[here] = value

        def message(k):
            p, peer = peer_of(k)
            return p, pltpu.make_async_remote_copy(
                src_ref=note.at[step], dst_ref=seen.at[here], send_sem=ssem.at[k - 1],
                recv_sem=rsem.at[here], device_id=peer, device_id_type=MESH)

        for k in range(1, 16):
            message(k)[1].start()
        for k in range(1, 16):
            p, _ = peer_of(k)
            pltpu.make_async_remote_copy(
                src_ref=note.at[step], dst_ref=seen.at[p], send_sem=ssem.at[k - 1],
                recv_sem=rsem.at[p], device_id=peer_of(k)[1], device_id_type=MESH).wait_recv()
        value = jnp.sum(seen[...], axis=0)
    norm[...] = jnp.sqrt(value / jnp.float32(entries))
    norm_copy = pltpu.make_async_copy(norm, norm_out, norm_sem)
    norm_copy.start()

    for step, (peer_of, seen, ssem, rsem, here) in enumerate((
            (line_peer, seen1, note1_send, note1_recv, line),
            (plane_peer, seen2, note2_send, note2_recv, plane))):
        for k in range(1, 16):
            pltpu.make_async_remote_copy(
                src_ref=note.at[step], dst_ref=seen.at[here], send_sem=ssem.at[k - 1],
                recv_sem=rsem.at[here], device_id=peer_of(k)[1], device_id_type=MESH).wait_send()

    def drain(k, _):
        for copy in copies(k, 1):
            copy.wait_send()
        return 0

    with jax.named_scope("drain"):
        lax.fori_loop(0, 12, drain, 0)
    out.wait()
    norm_copy.wait()


def write(avg, norm, avg_hbm, norm_out, sem):
    copy = pltpu.make_async_copy(avg, avg_hbm, sem)
    copy.start()
    norm_out[...] = norm[0, :norm_out.shape[0]]
    copy.wait()


def on_device(snapshots, coeffs):
    widths, snaps = coeffs.shape
    _, rows, all_cols = snapshots.shape
    cols = all_cols // 4
    entries = rows * all_cols * 64
    pieces = 16
    averages, norms = pl.pallas_call(
        functools.partial(kernel, (widths, snaps, cols, entries)),
        out_shape=(pltpu.VMEM((widths, rows, cols), jnp.float32), pltpu.VMEM((1, 128), jnp.float32)),
        in_specs=[pl.BlockSpec(memory_space=pl.ANY)] * 2,
        out_specs=[pl.BlockSpec(memory_space=pl.ANY)] * 2,
        scratch_shapes=[
            pltpu.VMEM((widths, rows, cols), jnp.float32),
            pltpu.VMEM((1, 128), jnp.float32),
            pltpu.VMEM((widths, snaps), jnp.float32),
            pltpu.VMEM((pieces, snaps, ROWS, cols), jnp.bfloat16),
            pltpu.VMEM((2 * widths * ROWS, snaps * ROWS), jnp.bfloat16),
            pltpu.VMEM((12, widths, ROWS, cols), jnp.bfloat16),
            pltpu.VMEM((12, 1, cols), jnp.float32),
            pltpu.VMEM((12, widths, ROWS, cols), jnp.bfloat16),
            pltpu.VMEM((12, 1, cols), jnp.float32),
            pltpu.VMEM((widths, cols), jnp.float32),
            pltpu.VMEM((2, 1, 128), jnp.float32),
            pltpu.VMEM((16, 1, 128), jnp.float32),
            pltpu.VMEM((16, 1, 128), jnp.float32),
            pltpu.SemaphoreType.DMA,
            pltpu.SemaphoreType.DMA((pieces,)),
            pltpu.SemaphoreType.DMA,
            pltpu.SemaphoreType.DMA,
            pltpu.SemaphoreType.REGULAR,
            pltpu.SemaphoreType.DMA((12,)),
            pltpu.SemaphoreType.DMA((12,)),
            pltpu.SemaphoreType.DMA((12,)),
            pltpu.SemaphoreType.DMA((12,)),
            pltpu.SemaphoreType.DMA((15,)),
            pltpu.SemaphoreType.DMA((16,)),
            pltpu.SemaphoreType.DMA((15,)),
            pltpu.SemaphoreType.DMA((16,)),
        ],
        compiler_params=pltpu.CompilerParams(collective_id=0, has_side_effects=True),
    )(coeffs, snapshots)
    return pl.pallas_call(
        write,
        out_shape=(jax.ShapeDtypeStruct((widths, rows, cols), jnp.float32),
                   jax.ShapeDtypeStruct((widths,), jnp.float32)),
        in_specs=[pl.BlockSpec(memory_space=pl.ANY), pl.BlockSpec(memory_space=pltpu.VMEM)],
        out_specs=(pl.BlockSpec(memory_space=pl.ANY), pl.BlockSpec(memory_space=pltpu.VMEM)),
        scratch_shapes=[pltpu.SemaphoreType.DMA],
    )(pltpu.with_memory_space_constraint(averages, pltpu.VMEM),
      pltpu.with_memory_space_constraint(norms, pltpu.VMEM))


def solution(mesh):
    split = Mesh(mesh.devices.reshape(mesh.shape["snap"], 2, 4, 4, 2), ("snap",) + PARAM)
    return jax.shard_map(
        on_device,
        mesh=split,
        in_specs=(P("snap", PARAM, None), P(None, "snap")),
        out_specs=(P(None, PARAM, "snap"), P()),
        check_vma=False,
    )
```

```python
import functools

import jax
import jax.numpy as jnp
from jax import lax
from jax.experimental import pallas as pl
from jax.experimental.pallas import tpu as pltpu
from jax.sharding import Mesh
from jax.sharding import PartitionSpec as P

MESH = pl.DeviceIdType.MESH
PARAM = ("zlo", "x", "y", "core")
ROWS = 16
HALF = 8
LEAST = -125.0
SPAN = 251.5
TINY = 1e-37
PIECES = 12
Z_FAR = (4, 3, -3, 2, -2, 1, -1, 0)
PLANE_FAR = tuple(sorted(((dx, dy) for dx in (-1, 0, 1, 2) for dy in (-1, 0, 1, 2)),
                         key=lambda d: -abs(d[0]) - abs(d[1])))


def encode(value):
    size = jnp.abs(value)
    largest = jnp.max(jnp.max(jnp.max(size, axis=0), axis=0), axis=0, keepdims=True)[None]
    largest = jnp.maximum(largest, TINY)
    inverse = 1.0 / largest
    power = jnp.exp2((size * inverse[:, None]) * SPAN + LEAST)
    return jnp.where(value < 0, -power, power).astype(jnp.bfloat16), largest


def decode(codes, largest):
    code = codes.astype(jnp.float32)
    size = (jnp.log2(jnp.abs(code)) - LEAST) * (largest * (1.0 / SPAN))[:, None]
    return jnp.where(code < 0, -size, size)


def tile_of(i):
    return (i % 2) * 2 + i // 2, 2 * (i % 2) - 1


def kernel(sizes, coeffs_hbm, snap_hbm, avg_out, norm_out,
           avg, norm, coef, stage, kron, sent, sent_max, got, got_max, piece, squares,
           note, seen1, seen2,
           coef_sem, stage_sem, out_sem, norm_sem, relay_sem, send_sem, send_max_sem,
           recv_sem, note_send, note_recv):
    widths, snaps, cols, entries = sizes
    halves = widths // HALF
    q = lax.axis_index("snap")
    zlo, x, y, core = (lax.axis_index(a) for a in PARAM)
    line = (q * 2 + zlo) * 2 + core
    plane = x * 4 + y

    def line_at(dz, to_core):
        z = (q * 2 + zlo + dz + 8) % 8
        return {"snap": z // 2, "zlo": z % 2, "core": to_core}

    def plane_at(dx, dy, to_core):
        return {"x": (x + dx + 4) % 4, "y": (y + dy + 4) % 4, "core": to_core}

    barrier = pltpu.get_barrier_semaphore()

    def load(k, group):
        kind, i = k // 4, k % 4
        tile, way = tile_of(i)
        block = (q + jnp.where(kind == 0, 2, jnp.where(kind == 1, 4 - way, jnp.where(kind == 2, 4 + way, 0)))) % 4
        return pltpu.make_async_copy(
            snap_hbm.at[:, pl.ds(pl.multiple_of(tile * ROWS, ROWS), ROWS),
                        pl.ds(pl.multiple_of(block * cols, cols), cols)],
            stage.at[k], stage_sem.at[group])

    coef_copy = pltpu.make_async_copy(coeffs_hbm, coef, coef_sem)
    coef_copy.start()
    load(0, 0).start()
    load(1, 1).start()
    near = [line_at(dz, core if same else 1 - core)
            for dz in (-2, 2, -1, 1, 0) for same in (True, False) if dz or not same]
    near += [plane_at(dx, dy, core if same else 1 - core)
             for dx, dy in PLANE_FAR if 0 < abs(dx) + abs(dy) <= 2 for same in (True, False)]
    for peer in near:
        pl.semaphore_signal(barrier, inc=1, device_id=peer, device_id_type=MESH)
    for k in range(2, 16):
        load(k, 2 + (k > 3) + (k > 7) + (k > 11)).start()

    m, n = HALF * ROWS, snaps * ROWS
    across = jnp.where(lax.broadcasted_iota(jnp.int32, (snaps, n), 1) // ROWS
                       == lax.broadcasted_iota(jnp.int32, (snaps, n), 0), 1.0, 0.0).astype(jnp.bfloat16)
    same = jnp.where(lax.broadcasted_iota(jnp.int32, (m, n), 0) % ROWS
                     == lax.broadcasted_iota(jnp.int32, (m, n), 1) % ROWS, 1.0, 0.0).astype(jnp.bfloat16)
    with jax.named_scope("coef_wait"):
        coef_copy.wait()
    part = jnp.broadcast_to(coef[...][:, None, :], (widths, ROWS, snaps)).reshape(widths * ROWS, snaps)
    for p in range(2):
        top = part.astype(jnp.bfloat16)
        part = part - top.astype(jnp.float32)
        spread = jnp.dot(top, across, preferred_element_type=jnp.float32).astype(jnp.bfloat16)
        for h in range(halves):
            kron[pl.ds((h * 2 + p) * m, m), :] = spread[h * m:(h + 1) * m] * same

    def product(k):
        both = jnp.dot(kron[...], stage[k].reshape(n, cols), preferred_element_type=jnp.float32)
        both = both.reshape(halves, 2, HALF, ROWS, cols)
        return both[:, 0] + both[:, 1]

    def copies(k, target):
        peer = {"snap": (q + target + 4) % 4}
        return (
            pltpu.make_async_remote_copy(
                src_ref=sent_max.at[k], dst_ref=got_max.at[k], send_sem=send_max_sem,
                recv_sem=recv_sem.at[k], device_id=peer, device_id_type=MESH),
            pltpu.make_async_remote_copy(
                src_ref=sent.at[k], dst_ref=got.at[k], send_sem=send_sem,
                recv_sem=recv_sem.at[k], device_id=peer, device_id_type=MESH),
        )

    def put(k, value):
        sent[k], sent_max[k] = encode(value)

    def send(k, target):
        for copy in copies(k, target):
            copy.start()

    def receive(k):
        pltpu.make_async_copy(piece, piece, recv_sem.at[k]).wait()
        return decode(got[k], got_max[k]).reshape(widths, ROWS, cols)

    load(0, 0).wait()
    put(0, product(0))
    with jax.named_scope("barrier"):
        pl.semaphore_wait(barrier, len(near))
    send(0, -1)

    def first(k, _):
        tile, way = tile_of(k % 4)
        put(k, product(k))
        send(k, jnp.where(k < 4, way, -way))
        return 0

    def loaded(k, count, group):
        pltpu.make_async_copy(stage.at[pl.ds(k, count)], stage.at[pl.ds(k, count)], stage_sem.at[group]).wait()

    with jax.named_scope("first"):
        load(1, 1).wait()
        lax.fori_loop(1, 2, first, 0)
        loaded(2, 2, 2)
        lax.fori_loop(2, 4, first, 0)
        loaded(4, 4, 3)
        lax.fori_loop(4, 8, first, 0)

    relays = [line_at(-2, core), line_at(2, core), plane_at(2, 0, core), plane_at(0, 2, core)]
    for peer in relays:
        pl.semaphore_signal(relay_sem, inc=1, device_id=peer, device_id_type=MESH)

    def rows_of(i):
        return pl.ds(pl.multiple_of(tile_of(i)[0] * ROWS, ROWS), ROWS)

    def mine(i, _):
        avg[:, rows_of(i), :] = product(12 + i).reshape(widths, ROWS, cols)
        return 0

    loaded(8, 4, 4)
    loaded(12, 4, 5)
    with jax.named_scope("mine"):
        lax.fori_loop(0, 4, mine, 0)

    def forward(i, _):
        tile, way = tile_of(i)
        put(8 + i, product(8 + i) + receive(i).reshape(halves, HALF, ROWS, cols))
        send(8 + i, way)
        return 0

    with jax.named_scope("forward"):
        lax.fori_loop(0, 4, forward, 0)

    def direct(i, _):
        avg[:, rows_of(i), :] += receive(4 + i)
        return 0

    with jax.named_scope("direct"):
        lax.fori_loop(0, 4, direct, 0)
    squares[...] = jnp.zeros_like(squares)
    with jax.named_scope("relay"):
        pl.semaphore_wait(relay_sem, len(relays))

    def last(i, _):
        value = avg[:, rows_of(i), :] + receive(8 + i)
        avg[:, rows_of(i), :] = value
        squares[...] += jnp.sum(value * value, axis=1)
        return 0

    with jax.named_scope("last"):
        lax.fori_loop(0, 4, last, 0)
    out = pltpu.make_async_copy(avg, avg_out, out_sem)
    out.start()

    per = jnp.sum(squares[...], axis=1, keepdims=True)
    spot = (lax.broadcasted_iota(jnp.int32, (widths, 128), 0)
            == lax.broadcasted_iota(jnp.int32, (widths, 128), 1))
    value = jnp.sum(jnp.where(spot, per, 0.0), axis=0, keepdims=True)
    note[0] = value
    seen1[line] = value

    def message(step, seen, here, peer):
        return pltpu.make_async_remote_copy(
            src_ref=note.at[step], dst_ref=seen.at[here], send_sem=note_send.at[step],
            recv_sem=note_recv.at[step], device_id=peer, device_id_type=MESH)

    def landed(step, count):
        return pltpu.make_async_copy(seen2.at[pl.ds(0, count)], seen2.at[pl.ds(0, count)], note_recv.at[step])

    def left(step, count):
        return pltpu.make_async_copy(seen2.at[pl.ds(0, count)], seen2.at[pl.ds(0, count)], note_send.at[step])

    hub = core == 1
    for dz in Z_FAR[:-1]:
        message(0, seen1, line, line_at(dz, 1)).start()

    @pl.when(jnp.logical_not(hub))
    def _():
        message(0, seen1, line, line_at(0, 1)).start()

    with jax.named_scope("drain"):
        pltpu.make_async_copy(sent, sent, send_sem).wait()
        pltpu.make_async_copy(sent_max, sent_max, send_max_sem).wait()

    @pl.when(hub)
    def _():
        with jax.named_scope("norm0"):
            landed(0, 15).wait()
        total = jnp.sum(seen1[...], axis=0)
        note[1] = total
        seen2[plane] = total
        for dx, dy in PLANE_FAR[:-1]:
            for to in (0, 1):
                message(1, seen2, plane, plane_at(dx, dy, to)).start()
        message(1, seen2, plane, plane_at(0, 0, 0)).start()
        left(0, 7).wait()
        with jax.named_scope("norm1"):
            landed(1, 15).wait()

    @pl.when(jnp.logical_not(hub))
    def _():
        left(0, 8).wait()
        with jax.named_scope("norm1"):
            landed(1, 16).wait()

    norm[...] = jnp.sqrt(jnp.sum(seen2[...], axis=0) / jnp.float32(entries))[0, :widths]
    norm_copy = pltpu.make_async_copy(norm, norm_out, norm_sem)
    norm_copy.start()

    @pl.when(hub)
    def _():
        left(1, 16).wait()
        left(1, 15).wait()

    out.wait()
    norm_copy.wait()


def write(avg, norm, avg_hbm, norm_hbm, sems):
    large = pltpu.make_async_copy(avg, avg_hbm, sems.at[0])
    small = pltpu.make_async_copy(norm, norm_hbm, sems.at[1])
    large.start()
    small.start()
    small.wait()
    large.wait()


def on_device(snapshots, coeffs):
    widths, snaps = coeffs.shape
    _, rows, all_cols = snapshots.shape
    cols = all_cols // 4
    halves = widths // HALF
    entries = rows * all_cols * 64
    averages, norms = pl.pallas_call(
        functools.partial(kernel, (widths, snaps, cols, entries)),
        out_shape=(pltpu.VMEM((widths, rows, cols), jnp.float32), pltpu.VMEM((widths,), jnp.float32)),
        in_specs=[pl.BlockSpec(memory_space=pl.ANY)] * 2,
        out_specs=[pl.BlockSpec(memory_space=pl.ANY)] * 2,
        scratch_shapes=[
            pltpu.VMEM((widths, rows, cols), jnp.float32),
            pltpu.VMEM((widths,), jnp.float32),
            pltpu.VMEM((widths, snaps), jnp.float32),
            pltpu.VMEM((16, snaps, ROWS, cols), jnp.bfloat16),
            pltpu.VMEM((2 * widths * ROWS, snaps * ROWS), jnp.bfloat16),
            pltpu.VMEM((PIECES, halves, HALF, ROWS, cols), jnp.bfloat16),
            pltpu.VMEM((PIECES, 1, 1, cols), jnp.float32),
            pltpu.VMEM((PIECES, halves, HALF, ROWS, cols), jnp.bfloat16),
            pltpu.VMEM((PIECES, 1, 1, cols), jnp.float32),
            pltpu.VMEM((widths * ROWS // 2 + 1, 1, cols), jnp.float32),
            pltpu.VMEM((widths, cols), jnp.float32),
            pltpu.VMEM((2, 1, 128), jnp.float32),
            pltpu.VMEM((16, 1, 128), jnp.float32),
            pltpu.VMEM((16, 1, 128), jnp.float32),
            pltpu.SemaphoreType.DMA,
            pltpu.SemaphoreType.DMA((6,)),
            pltpu.SemaphoreType.DMA,
            pltpu.SemaphoreType.DMA,
            pltpu.SemaphoreType.REGULAR,
            pltpu.SemaphoreType.DMA,
            pltpu.SemaphoreType.DMA,
            pltpu.SemaphoreType.DMA((PIECES,)),
            pltpu.SemaphoreType.DMA((2,)),
            pltpu.SemaphoreType.DMA((2,)),
        ],
        compiler_params=pltpu.CompilerParams(collective_id=0, has_side_effects=True),
    )(coeffs, snapshots)
    return pl.pallas_call(
        write,
        out_shape=(jax.ShapeDtypeStruct((widths, rows, cols), jnp.float32),
                   jax.ShapeDtypeStruct((widths,), jnp.float32)),
        in_specs=[pl.BlockSpec(memory_space=pl.ANY)] * 2,
        out_specs=[pl.BlockSpec(memory_space=pl.ANY)] * 2,
        scratch_shapes=[pltpu.SemaphoreType.DMA((2,))],
    )(pltpu.with_memory_space_constraint(averages, pltpu.VMEM),
      pltpu.with_memory_space_constraint(norms, pltpu.VMEM))


def solution(mesh):
    split = Mesh(mesh.devices.reshape(mesh.shape["snap"], 2, 4, 4, 2), ("snap",) + PARAM)
    return jax.shard_map(
        on_device,
        mesh=split,
        in_specs=(P("snap", PARAM, None), P(None, "snap")),
        out_specs=(P(None, PARAM, "snap"), P()),
        check_vma=False,
    )
```

```python
import functools

import jax
import jax.numpy as jnp
from jax import lax
from jax.experimental import pallas as pl
from jax.experimental.pallas import tpu as pltpu
from jax.sharding import Mesh
from jax.sharding import PartitionSpec as P

MESH = pl.DeviceIdType.MESH
PARAM = ("zlo", "x", "y", "core")
ROWS = 16
HALF = 8
LEAST = -125.0
SPAN = 251.5
TINY = 1e-37
PIECES = 12
EARLY = ((0, 0, 0, 1),)
Z_FAR = (4, 3, -3, 2, -2, 1, -1, 0)
PLANE_FAR = tuple(sorted(((dx, dy) for dx in (-1, 0, 1, 2) for dy in (-1, 0, 1, 2)),
                         key=lambda d: -abs(d[0]) - abs(d[1])))


def encode(value):
    size = jnp.abs(value)
    largest = jnp.max(jnp.max(jnp.max(size, axis=0), axis=0), axis=0, keepdims=True)[None]
    largest = jnp.maximum(largest, TINY)
    inverse = 1.0 / largest
    power = jnp.exp2((size * inverse[:, None]) * SPAN + LEAST)
    return jnp.where(value < 0, -power, power).astype(jnp.bfloat16), largest


def decode(codes, largest):
    code = codes.astype(jnp.float32)
    size = (jnp.log2(jnp.abs(code)) - LEAST) * (largest * (1.0 / SPAN))[:, None]
    return jnp.where(code < 0, -size, size)


def tile_of(i):
    return (i % 2) * 2 + i // 2, 2 * (i % 2) - 1


def kernel(sizes, coeffs_hbm, snap_hbm, avg_out, norm_out,
           avg, norm, coef, stage, kron, sent, sent_max, got, got_max, piece, squares,
           note, seen1, seen2, seen,
           coef_sem, stage_sem, out_sem, norm_sem, relay_sem, all_sem, send_sem, send_max_sem,
           recv_sem, note_send, note_recv):
    widths, snaps, cols, entries = sizes
    halves = widths // HALF
    q = lax.axis_index("snap")
    zlo, x, y, core = (lax.axis_index(a) for a in PARAM)
    line = (q * 2 + zlo) * 2 + core
    plane = x * 4 + y
    z = q * 2 + zlo

    def line_at(dz, to_core):
        z = (q * 2 + zlo + dz + 8) % 8
        return {"snap": z // 2, "zlo": z % 2, "core": to_core}

    def plane_at(dx, dy, to_core):
        return {"x": (x + dx + 4) % 4, "y": (y + dy + 4) % 4, "core": to_core}

    barrier = pltpu.get_barrier_semaphore()

    def load(k, group):
        kind, i = k // 4, k % 4
        tile, way = tile_of(i)
        block = (q + jnp.where(kind == 0, 2, jnp.where(kind == 1, 4 - way, jnp.where(kind == 2, 4 + way, 0)))) % 4
        return pltpu.make_async_copy(
            snap_hbm.at[:, pl.ds(pl.multiple_of(tile * ROWS, ROWS), ROWS),
                        pl.ds(pl.multiple_of(block * cols, cols), cols)],
            stage.at[k], stage_sem.at[group])

    coef_copy = pltpu.make_async_copy(coeffs_hbm, coef, coef_sem)
    coef_copy.start()
    load(0, 0).start()
    load(1, 1).start()
    near = [line_at(dz, core if same else 1 - core)
            for dz in (-2, 2, -1, 1, 0) for same in (True, False) if dz or not same]
    near += [plane_at(dx, dy, core if same else 1 - core)
             for dx, dy in PLANE_FAR if 0 < abs(dx) + abs(dy) <= 2 for same in (True, False)]
    for peer in near:
        pl.semaphore_signal(barrier, inc=1, device_id=peer, device_id_type=MESH)
    for k in range(2, 16):
        load(k, 2 + (k > 3) + (k > 7) + (k > 11)).start()

    m, n = HALF * ROWS, snaps * ROWS
    across = jnp.where(lax.broadcasted_iota(jnp.int32, (snaps, n), 1) // ROWS
                       == lax.broadcasted_iota(jnp.int32, (snaps, n), 0), 1.0, 0.0).astype(jnp.bfloat16)
    same = jnp.where(lax.broadcasted_iota(jnp.int32, (m, n), 0) % ROWS
                     == lax.broadcasted_iota(jnp.int32, (m, n), 1) % ROWS, 1.0, 0.0).astype(jnp.bfloat16)
    with jax.named_scope("coef_wait"):
        coef_copy.wait()
    part = jnp.broadcast_to(coef[...][:, None, :], (widths, ROWS, snaps)).reshape(widths * ROWS, snaps)
    for p in range(2):
        top = part.astype(jnp.bfloat16)
        part = part - top.astype(jnp.float32)
        spread = jnp.dot(top, across, preferred_element_type=jnp.float32).astype(jnp.bfloat16)
        for h in range(halves):
            kron[pl.ds((h * 2 + p) * m, m), :] = spread[h * m:(h + 1) * m] * same

    def product(k):
        both = jnp.dot(kron[...], stage[k].reshape(n, cols), preferred_element_type=jnp.float32)
        both = both.reshape(halves, 2, HALF, ROWS, cols)
        return both[:, 0] + both[:, 1]

    def copies(k, target):
        peer = {"snap": (q + target + 4) % 4}
        return (
            pltpu.make_async_remote_copy(
                src_ref=sent_max.at[k], dst_ref=got_max.at[k], send_sem=send_max_sem,
                recv_sem=recv_sem.at[k], device_id=peer, device_id_type=MESH),
            pltpu.make_async_remote_copy(
                src_ref=sent.at[k], dst_ref=got.at[k], send_sem=send_sem,
                recv_sem=recv_sem.at[k], device_id=peer, device_id_type=MESH),
        )

    def put(k, value):
        sent[k], sent_max[k] = encode(value)

    def send(k, target):
        for copy in copies(k, target):
            copy.start()

    def receive(k):
        pltpu.make_async_copy(piece, piece, recv_sem.at[k]).wait()
        return decode(got[k], got_max[k]).reshape(widths, ROWS, cols)

    load(0, 0).wait()
    put(0, product(0))
    with jax.named_scope("barrier"):
        pl.semaphore_wait(barrier, len(near))
    send(0, -1)

    def first(k, _):
        tile, way = tile_of(k % 4)
        put(k, product(k))
        send(k, jnp.where(k < 4, way, -way))
        return 0

    def loaded(k, count, group):
        pltpu.make_async_copy(stage.at[pl.ds(k, count)], stage.at[pl.ds(k, count)], stage_sem.at[group]).wait()

    with jax.named_scope("first"):
        load(1, 1).wait()
        lax.fori_loop(1, 2, first, 0)
        loaded(2, 2, 2)
        lax.fori_loop(2, 4, first, 0)
        loaded(4, 4, 3)
        lax.fori_loop(4, 8, first, 0)

    relays = [line_at(-2, core), line_at(2, core), plane_at(2, 0, core), plane_at(0, 2, core)]
    for peer in relays:
        pl.semaphore_signal(relay_sem, inc=1, device_id=peer, device_id_type=MESH)

    def rows_of(i):
        return pl.ds(pl.multiple_of(tile_of(i)[0] * ROWS, ROWS), ROWS)

    def mine(i, _):
        avg[:, rows_of(i), :] = product(12 + i).reshape(widths, ROWS, cols)
        return 0

    loaded(8, 4, 4)
    loaded(12, 4, 5)
    with jax.named_scope("mine"):
        lax.fori_loop(0, 4, mine, 0)

    def forward(i, _):
        tile, way = tile_of(i)
        put(8 + i, product(8 + i) + receive(i).reshape(halves, HALF, ROWS, cols))
        send(8 + i, way)
        return 0

    with jax.named_scope("forward"):
        lax.fori_loop(0, 4, forward, 0)

    pl.semaphore_wait(relay_sem, len(relays))
    for dx, dy in PLANE_FAR[:-1]:
        pl.semaphore_signal(all_sem, inc=1, device_id=plane_at(dx, dy, core), device_id_type=MESH)

    def direct(i, _):
        avg[:, rows_of(i), :] += receive(4 + i)
        return 0

    with jax.named_scope("direct"):
        lax.fori_loop(0, 4, direct, 0)
    squares[...] = jnp.zeros_like(squares)
    with jax.named_scope("relay"):
        pl.semaphore_wait(all_sem, len(PLANE_FAR) - 1)

    def last(i, _):
        value = avg[:, rows_of(i), :] + receive(8 + i)
        avg[:, rows_of(i), :] = value
        squares[...] += jnp.sum(value * value, axis=1)
        return 0

    with jax.named_scope("last"):
        lax.fori_loop(0, 4, last, 0)
    out = pltpu.make_async_copy(avg, avg_out, out_sem)
    out.start()

    per = jnp.sum(squares[...], axis=1, keepdims=True)
    spot = (lax.broadcasted_iota(jnp.int32, (widths, 128), 0)
            == lax.broadcasted_iota(jnp.int32, (widths, 128), 1))
    value = jnp.sum(jnp.where(spot, per, 0.0), axis=0, keepdims=True)
    note[0] = value
    seen1[line] = value

    def message(step, there, here, peer):
        return pltpu.make_async_remote_copy(
            src_ref=note.at[step % 2], dst_ref=there.at[here], send_sem=note_send.at[step],
            recv_sem=note_recv.at[step], device_id=peer, device_id_type=MESH)

    def wait(sem, count):
        pltpu.make_async_copy(seen.at[pl.ds(0, count)], seen.at[pl.ds(0, count)], sem).wait()

    def line_sum(there, first):
        total = there[first]
        for i in range(1, 16):
            total = total + there[first + i]
        return total

    hub = core == 1
    early = [(z == ez) & (x == ex) & (y == ey) & (core == ec) for ez, ex, ey, ec in EARLY]
    is_early = functools.reduce(jnp.logical_or, early)
    for me, (ez, ex, ey, ec) in zip(early, EARLY):
        @pl.when(jnp.logical_not(me))
        def _():
            message(2, seen, plane * 16 + line,
                    {"snap": ez // 2, "zlo": ez % 2, "x": ex, "y": ey, "core": ec}).start()
    for dz in Z_FAR[:-1]:
        message(0, seen1, line, line_at(dz, 1)).start()

    @pl.when(jnp.logical_not(hub))
    def _():
        message(0, seen1, line, line_at(0, 1)).start()

    with jax.named_scope("drain"):
        pltpu.make_async_copy(sent, sent, send_sem).wait()
        pltpu.make_async_copy(sent_max, sent_max, send_max_sem).wait()

    def spread(skip):
        for dx, dy in PLANE_FAR:
            for to in (0, 1):
                if (dx, dy) == (0, 0) and to == 1:
                    continue
                peer = plane_at(dx, dy, to)
                known = [(z == ez) & (peer["x"] == ex) & (peer["y"] == ey) for ez, ex, ey, ec in EARLY if ec == to]
                if skip and known:
                    @pl.when(jnp.logical_not(functools.reduce(jnp.logical_or, known)))
                    def _():
                        message(1, seen2, plane, peer).start()
                else:
                    message(1, seen2, plane, peer).start()

    planes = sorted({e[0] for e in EARLY})
    early_plane = functools.reduce(jnp.logical_or, [z == ez for ez in planes])

    @pl.when(hub)
    def _():
        with jax.named_scope("norm0"):
            wait(note_recv.at[0], 15)
        total = line_sum(seen1, 0)
        note[1] = total
        seen2[plane] = total

        @pl.when(early_plane)
        def _():
            spread(True)

        @pl.when(jnp.logical_not(early_plane))
        def _():
            spread(False)

    @pl.when(is_early)
    def _():
        seen[plane * 16 + line] = value
        with jax.named_scope("norm2"):
            wait(note_recv.at[2], 255)
        for p in range(16):
            seen2[p] = line_sum(seen, p * 16)

    @pl.when(jnp.logical_not(is_early) & hub)
    def _():
        with jax.named_scope("norm1"):
            wait(note_recv.at[1], 15)

    @pl.when(jnp.logical_not(is_early | hub))
    def _():
        with jax.named_scope("norm1"):
            wait(note_recv.at[1], 16)

    norm[...] = jnp.sqrt(jnp.sum(seen2[...], axis=0) / jnp.float32(entries))[0, :widths]
    norm_copy = pltpu.make_async_copy(norm, norm_out, norm_sem)
    norm_copy.start()

    @pl.when(hub)
    def _():
        wait(note_send.at[0], 7)
        for ez in planes:
            @pl.when(z == ez)
            def _():
                others = [e for e in EARLY if e[0] == ez]
                for me, e in zip(early, EARLY):
                    if e in others and e[3] == 1:
                        @pl.when(me)
                        def _():
                            wait(note_send.at[1], 31 - len(others) + 1)
                hubs = [me for me, e in zip(early, EARLY) if e in others and e[3] == 1]
                if hubs:
                    @pl.when(jnp.logical_not(functools.reduce(jnp.logical_or, hubs)))
                    def _():
                        wait(note_send.at[1], 31 - len(others))
                else:
                    wait(note_send.at[1], 31 - len(others))

        @pl.when(jnp.logical_not(early_plane))
        def _():
            wait(note_send.at[1], 31)

    @pl.when(jnp.logical_not(hub))
    def _():
        wait(note_send.at[0], 8)

    @pl.when(is_early)
    def _():
        if len(EARLY) > 1:
            wait(note_send.at[2], len(EARLY) - 1)

    @pl.when(jnp.logical_not(is_early))
    def _():
        wait(note_send.at[2], len(EARLY))

    out.wait()
    norm_copy.wait()


def write(avg, norm, avg_hbm, norm_hbm, sems):
    large = pltpu.make_async_copy(avg, avg_hbm, sems.at[0])
    small = pltpu.make_async_copy(norm, norm_hbm, sems.at[1])
    large.start()
    small.start()
    small.wait()
    large.wait()


def on_device(snapshots, coeffs):
    widths, snaps = coeffs.shape
    _, rows, all_cols = snapshots.shape
    cols = all_cols // 4
    halves = widths // HALF
    entries = rows * all_cols * 64
    averages, norms = pl.pallas_call(
        functools.partial(kernel, (widths, snaps, cols, entries)),
        out_shape=(pltpu.VMEM((widths, rows, cols), jnp.float32), pltpu.VMEM((widths,), jnp.float32)),
        in_specs=[pl.BlockSpec(memory_space=pl.ANY)] * 2,
        out_specs=[pl.BlockSpec(memory_space=pl.ANY)] * 2,
        scratch_shapes=[
            pltpu.VMEM((widths, rows, cols), jnp.float32),
            pltpu.VMEM((widths,), jnp.float32),
            pltpu.VMEM((widths, snaps), jnp.float32),
            pltpu.VMEM((16, snaps, ROWS, cols), jnp.bfloat16),
            pltpu.VMEM((2 * widths * ROWS, snaps * ROWS), jnp.bfloat16),
            pltpu.VMEM((PIECES, halves, HALF, ROWS, cols), jnp.bfloat16),
            pltpu.VMEM((PIECES, 1, 1, cols), jnp.float32),
            pltpu.VMEM((PIECES, halves, HALF, ROWS, cols), jnp.bfloat16),
            pltpu.VMEM((PIECES, 1, 1, cols), jnp.float32),
            pltpu.VMEM((widths * ROWS // 2 + 1, 1, cols), jnp.float32),
            pltpu.VMEM((widths, cols), jnp.float32),
            pltpu.VMEM((2, 1, 128), jnp.float32),
            pltpu.VMEM((16, 1, 128), jnp.float32),
            pltpu.VMEM((16, 1, 128), jnp.float32),
            pltpu.VMEM((256, 1, 128), jnp.float32),
            pltpu.SemaphoreType.DMA,
            pltpu.SemaphoreType.DMA((6,)),
            pltpu.SemaphoreType.DMA,
            pltpu.SemaphoreType.DMA,
            pltpu.SemaphoreType.REGULAR,
            pltpu.SemaphoreType.REGULAR,
            pltpu.SemaphoreType.DMA,
            pltpu.SemaphoreType.DMA,
            pltpu.SemaphoreType.DMA((PIECES,)),
            pltpu.SemaphoreType.DMA((3,)),
            pltpu.SemaphoreType.DMA((3,)),
        ],
        compiler_params=pltpu.CompilerParams(collective_id=0, has_side_effects=True),
    )(coeffs, snapshots)
    return pl.pallas_call(
        write,
        out_shape=(jax.ShapeDtypeStruct((widths, rows, cols), jnp.float32),
                   jax.ShapeDtypeStruct((widths,), jnp.float32)),
        in_specs=[pl.BlockSpec(memory_space=pl.ANY)] * 2,
        out_specs=[pl.BlockSpec(memory_space=pl.ANY)] * 2,
        scratch_shapes=[pltpu.SemaphoreType.DMA((2,))],
    )(pltpu.with_memory_space_constraint(averages, pltpu.VMEM),
      pltpu.with_memory_space_constraint(norms, pltpu.VMEM))


def solution(mesh):
    split = Mesh(mesh.devices.reshape(mesh.shape["snap"], 2, 4, 4, 2), ("snap",) + PARAM)
    return jax.shard_map(
        on_device,
        mesh=split,
        in_specs=(P("snap", PARAM, None), P(None, "snap")),
        out_specs=(P(None, PARAM, "snap"), P()),
        check_vma=False,
    )
```

```python
import functools

import jax
import jax.numpy as jnp
from jax import lax
from jax.experimental import pallas as pl
from jax.experimental.pallas import tpu as pltpu
from jax.sharding import Mesh
from jax.sharding import PartitionSpec as P

MESH = pl.DeviceIdType.MESH
PARAM = ("zlo", "x", "y", "core")
ROWS = 16
HALF = 8
LEAST = -125.0
SPAN = 251.5
TINY = 1e-37
PIECES = 12
EARLY = ((0, 0, 0, 1), (1, 0, 0, 1), (1, 0, 0, 0))
Z_FAR = (4, 3, -3, 2, -2, 1, -1, 0)
PLANE_FAR = tuple(sorted(((dx, dy) for dx in (-1, 0, 1, 2) for dy in (-1, 0, 1, 2)),
                         key=lambda d: -abs(d[0]) - abs(d[1])))


def encode(value):
    size = jnp.abs(value)
    largest = jnp.max(jnp.max(jnp.max(size, axis=0), axis=0), axis=0, keepdims=True)[None]
    largest = jnp.maximum(largest, TINY)
    inverse = 1.0 / largest
    power = jnp.exp2((size * inverse[:, None]) * SPAN + LEAST)
    return jnp.where(value < 0, -power, power).astype(jnp.bfloat16), largest


def decode(codes, largest):
    code = codes.astype(jnp.float32)
    size = (jnp.log2(jnp.abs(code)) - LEAST) * (largest * (1.0 / SPAN))[:, None]
    return jnp.where(code < 0, -size, size)


def tile_of(i):
    return (i % 2) * 2 + i // 2, 2 * (i % 2) - 1


def kernel(sizes, coeffs_hbm, snap_hbm, avg_out, norm_out,
           avg, norm, coef, stage, kron, sent, sent_max, got, got_max, piece, squares,
           note, seen1, seen2, seen,
           coef_sem, stage_sem, out_sem, norm_sem, relay_sem, all_sem, send_sem, send_max_sem,
           recv_sem, note_send, note_recv):
    widths, snaps, cols, entries = sizes
    halves = widths // HALF
    q = lax.axis_index("snap")
    zlo, x, y, core = (lax.axis_index(a) for a in PARAM)
    line = (q * 2 + zlo) * 2 + core
    plane = x * 4 + y
    z = q * 2 + zlo

    def line_at(dz, to_core):
        z = (q * 2 + zlo + dz + 8) % 8
        return {"snap": z // 2, "zlo": z % 2, "core": to_core}

    def plane_at(dx, dy, to_core):
        return {"x": (x + dx + 4) % 4, "y": (y + dy + 4) % 4, "core": to_core}

    barrier = pltpu.get_barrier_semaphore()

    def load(k, group):
        kind, i = k // 4, k % 4
        tile, way = tile_of(i)
        block = (q + jnp.where(kind == 0, 2, jnp.where(kind == 1, 4 - way, jnp.where(kind == 2, 4 + way, 0)))) % 4
        return pltpu.make_async_copy(
            snap_hbm.at[:, pl.ds(pl.multiple_of(tile * ROWS, ROWS), ROWS),
                        pl.ds(pl.multiple_of(block * cols, cols), cols)],
            stage.at[k], stage_sem.at[group])

    coef_copy = pltpu.make_async_copy(coeffs_hbm, coef, coef_sem)
    coef_copy.start()
    load(0, 0).start()
    near = [line_at(dz, core if same else 1 - core)
            for dz in (-2, 2, -1, 1, 0) for same in (True, False) if dz or not same]
    near += [plane_at(dx, dy, core if same else 1 - core)
             for dx, dy in PLANE_FAR if 0 < abs(dx) + abs(dy) <= 2 for same in (True, False)]
    for peer in near:
        pl.semaphore_signal(barrier, inc=1, device_id=peer, device_id_type=MESH)
    for k in range(1, 16):
        load(k, 1 + (k > 3) + (k > 7) + (k > 11)).start()

    m, n = HALF * ROWS, snaps * ROWS
    across = jnp.where(lax.broadcasted_iota(jnp.int32, (snaps, n), 1) // ROWS
                       == lax.broadcasted_iota(jnp.int32, (snaps, n), 0), 1.0, 0.0).astype(jnp.bfloat16)
    same = jnp.where(lax.broadcasted_iota(jnp.int32, (m, n), 0) % ROWS
                     == lax.broadcasted_iota(jnp.int32, (m, n), 1) % ROWS, 1.0, 0.0).astype(jnp.bfloat16)
    with jax.named_scope("coef_wait"):
        coef_copy.wait()
    part = jnp.broadcast_to(coef[...][:, None, :], (widths, ROWS, snaps)).reshape(widths * ROWS, snaps)
    for p in range(2):
        top = part.astype(jnp.bfloat16)
        part = part - top.astype(jnp.float32)
        spread = jnp.dot(top, across, preferred_element_type=jnp.float32).astype(jnp.bfloat16)
        for h in range(halves):
            kron[pl.ds((h * 2 + p) * m, m), :] = spread[h * m:(h + 1) * m] * same

    def product(k):
        both = jnp.dot(kron[...], stage[k].reshape(n, cols), preferred_element_type=jnp.float32)
        both = both.reshape(halves, 2, HALF, ROWS, cols)
        return both[:, 0] + both[:, 1]

    def copies(k, target):
        peer = {"snap": (q + target + 4) % 4}
        return (
            pltpu.make_async_remote_copy(
                src_ref=sent_max.at[k], dst_ref=got_max.at[k], send_sem=send_max_sem,
                recv_sem=recv_sem.at[k], device_id=peer, device_id_type=MESH),
            pltpu.make_async_remote_copy(
                src_ref=sent.at[k], dst_ref=got.at[k], send_sem=send_sem,
                recv_sem=recv_sem.at[k], device_id=peer, device_id_type=MESH),
        )

    def put(k, value):
        sent[k], sent_max[k] = encode(value)

    def send(k, target):
        for copy in copies(k, target):
            copy.start()

    def receive(k):
        pltpu.make_async_copy(piece, piece, recv_sem.at[k]).wait()
        return decode(got[k], got_max[k]).reshape(widths, ROWS, cols)

    load(0, 0).wait()
    put(0, product(0))
    with jax.named_scope("barrier"):
        pl.semaphore_wait(barrier, len(near))
    send(0, -1)

    def first(k, _):
        tile, way = tile_of(k % 4)
        put(k, product(k))
        send(k, jnp.where(k < 4, way, -way))
        return 0

    def loaded(k, count, group):
        pltpu.make_async_copy(stage.at[pl.ds(k, count)], stage.at[pl.ds(k, count)], stage_sem.at[group]).wait()

    with jax.named_scope("first"):
        loaded(1, 3, 1)
        lax.fori_loop(1, 4, first, 0)
        loaded(4, 4, 2)
        lax.fori_loop(4, 8, first, 0)

    relays = [line_at(-2, core), line_at(2, core), plane_at(2, 0, core), plane_at(0, 2, core)]
    for peer in relays:
        pl.semaphore_signal(relay_sem, inc=1, device_id=peer, device_id_type=MESH)

    def rows_of(i):
        return pl.ds(pl.multiple_of(tile_of(i)[0] * ROWS, ROWS), ROWS)

    def mine(i, _):
        avg[:, rows_of(i), :] = product(12 + i).reshape(widths, ROWS, cols)
        return 0

    loaded(8, 4, 3)
    loaded(12, 4, 4)
    with jax.named_scope("mine"):
        lax.fori_loop(0, 4, mine, 0)

    def forward(i, _):
        tile, way = tile_of(i)
        put(8 + i, product(8 + i) + receive(i).reshape(halves, HALF, ROWS, cols))
        send(8 + i, way)
        return 0

    with jax.named_scope("forward"):
        lax.fori_loop(0, 4, forward, 0)

    pl.semaphore_wait(relay_sem, len(relays))
    for dx, dy in PLANE_FAR[:-1]:
        pl.semaphore_signal(all_sem, inc=1, device_id=plane_at(dx, dy, core), device_id_type=MESH)

    def direct(i, _):
        avg[:, rows_of(i), :] += receive(4 + i)
        return 0

    with jax.named_scope("direct"):
        lax.fori_loop(0, 4, direct, 0)
    squares[...] = jnp.zeros_like(squares)
    with jax.named_scope("relay"):
        pl.semaphore_wait(all_sem, len(PLANE_FAR) - 1)

    def last(i, _):
        value = avg[:, rows_of(i), :] + receive(8 + i)
        avg[:, rows_of(i), :] = value
        squares[...] += jnp.sum(value * value, axis=1)
        return 0

    with jax.named_scope("last"):
        lax.fori_loop(0, 4, last, 0)
    out = pltpu.make_async_copy(avg, avg_out, out_sem)
    out.start()

    per = jnp.sum(squares[...], axis=1, keepdims=True)
    spot = (lax.broadcasted_iota(jnp.int32, (widths, 128), 0)
            == lax.broadcasted_iota(jnp.int32, (widths, 128), 1))
    value = jnp.sum(jnp.where(spot, per, 0.0), axis=0, keepdims=True)
    note[0] = value
    seen1[line] = value

    def message(step, there, here, peer):
        return pltpu.make_async_remote_copy(
            src_ref=note.at[step % 2], dst_ref=there.at[here], send_sem=note_send.at[step],
            recv_sem=note_recv.at[step], device_id=peer, device_id_type=MESH)

    def wait(sem, count):
        pltpu.make_async_copy(seen.at[pl.ds(0, count)], seen.at[pl.ds(0, count)], sem).wait()

    def line_sum(there, first):
        total = there[first]
        for i in range(1, 16):
            total = total + there[first + i]
        return total

    hub = core == 1
    early = [(z == ez) & (x == ex) & (y == ey) & (core == ec) for ez, ex, ey, ec in EARLY]
    is_early = functools.reduce(jnp.logical_or, early)
    for me, (ez, ex, ey, ec) in zip(early, EARLY):
        @pl.when(jnp.logical_not(me))
        def _():
            message(2, seen, plane * 16 + line,
                    {"snap": ez // 2, "zlo": ez % 2, "x": ex, "y": ey, "core": ec}).start()
    for dz in Z_FAR[:-1]:
        message(0, seen1, line, line_at(dz, 1)).start()

    @pl.when(jnp.logical_not(hub))
    def _():
        message(0, seen1, line, line_at(0, 1)).start()

    with jax.named_scope("drain"):
        pltpu.make_async_copy(sent, sent, send_sem).wait()
        pltpu.make_async_copy(sent_max, sent_max, send_max_sem).wait()

    def spread(skip):
        for dx, dy in PLANE_FAR:
            for to in (0, 1):
                if (dx, dy) == (0, 0) and to == 1:
                    continue
                peer = plane_at(dx, dy, to)
                known = [(z == ez) & (peer["x"] == ex) & (peer["y"] == ey) for ez, ex, ey, ec in EARLY if ec == to]
                if skip and known:
                    @pl.when(jnp.logical_not(functools.reduce(jnp.logical_or, known)))
                    def _():
                        message(1, seen2, plane, peer).start()
                else:
                    message(1, seen2, plane, peer).start()

    planes = sorted({e[0] for e in EARLY})
    early_plane = functools.reduce(jnp.logical_or, [z == ez for ez in planes])

    @pl.when(hub)
    def _():
        with jax.named_scope("norm0"):
            wait(note_recv.at[0], 15)
        total = line_sum(seen1, 0)
        note[1] = total
        seen2[plane] = total

        @pl.when(early_plane)
        def _():
            spread(True)

        @pl.when(jnp.logical_not(early_plane))
        def _():
            spread(False)

    @pl.when(is_early)
    def _():
        seen[plane * 16 + line] = value
        with jax.named_scope("norm2"):
            wait(note_recv.at[2], 255)
        for p in range(16):
            seen2[p] = line_sum(seen, p * 16)

    @pl.when(jnp.logical_not(is_early) & hub)
    def _():
        with jax.named_scope("norm1"):
            wait(note_recv.at[1], 15)

    @pl.when(jnp.logical_not(is_early | hub))
    def _():
        with jax.named_scope("norm1"):
            wait(note_recv.at[1], 16)

    norm[...] = jnp.sqrt(jnp.sum(seen2[...], axis=0) / jnp.float32(entries))[0, :widths]
    norm_copy = pltpu.make_async_copy(norm, norm_out, norm_sem)
    norm_copy.start()

    @pl.when(hub)
    def _():
        wait(note_send.at[0], 7)
        for ez in planes:
            @pl.when(z == ez)
            def _():
                others = [e for e in EARLY if e[0] == ez]
                for me, e in zip(early, EARLY):
                    if e in others and e[3] == 1:
                        @pl.when(me)
                        def _():
                            wait(note_send.at[1], 31 - len(others) + 1)
                hubs = [me for me, e in zip(early, EARLY) if e in others and e[3] == 1]
                if hubs:
                    @pl.when(jnp.logical_not(functools.reduce(jnp.logical_or, hubs)))
                    def _():
                        wait(note_send.at[1], 31 - len(others))
                else:
                    wait(note_send.at[1], 31 - len(others))

        @pl.when(jnp.logical_not(early_plane))
        def _():
            wait(note_send.at[1], 31)

    @pl.when(jnp.logical_not(hub))
    def _():
        wait(note_send.at[0], 8)

    @pl.when(is_early)
    def _():
        if len(EARLY) > 1:
            wait(note_send.at[2], len(EARLY) - 1)

    @pl.when(jnp.logical_not(is_early))
    def _():
        wait(note_send.at[2], len(EARLY))

    out.wait()
    norm_copy.wait()


def write(avg, norm, avg_hbm, norm_hbm, sems):
    large = pltpu.make_async_copy(avg, avg_hbm, sems.at[0])
    small = pltpu.make_async_copy(norm, norm_hbm, sems.at[1])
    large.start()
    small.start()
    small.wait()
    large.wait()


def on_device(snapshots, coeffs):
    widths, snaps = coeffs.shape
    _, rows, all_cols = snapshots.shape
    cols = all_cols // 4
    halves = widths // HALF
    entries = rows * all_cols * 64
    averages, norms = pl.pallas_call(
        functools.partial(kernel, (widths, snaps, cols, entries)),
        out_shape=(pltpu.VMEM((widths, rows, cols), jnp.float32), pltpu.VMEM((widths,), jnp.float32)),
        in_specs=[pl.BlockSpec(memory_space=pl.ANY)] * 2,
        out_specs=[pl.BlockSpec(memory_space=pl.ANY)] * 2,
        scratch_shapes=[
            pltpu.VMEM((widths, rows, cols), jnp.float32),
            pltpu.VMEM((widths,), jnp.float32),
            pltpu.VMEM((widths, snaps), jnp.float32),
            pltpu.VMEM((16, snaps, ROWS, cols), jnp.bfloat16),
            pltpu.VMEM((2 * widths * ROWS, snaps * ROWS), jnp.bfloat16),
            pltpu.VMEM((PIECES, halves, HALF, ROWS, cols), jnp.bfloat16),
            pltpu.VMEM((PIECES, 1, 1, cols), jnp.float32),
            pltpu.VMEM((PIECES, halves, HALF, ROWS, cols), jnp.bfloat16),
            pltpu.VMEM((PIECES, 1, 1, cols), jnp.float32),
            pltpu.VMEM((widths * ROWS // 2 + 1, 1, cols), jnp.float32),
            pltpu.VMEM((widths, cols), jnp.float32),
            pltpu.VMEM((2, 1, 128), jnp.float32),
            pltpu.VMEM((16, 1, 128), jnp.float32),
            pltpu.VMEM((16, 1, 128), jnp.float32),
            pltpu.VMEM((256, 1, 128), jnp.float32),
            pltpu.SemaphoreType.DMA,
            pltpu.SemaphoreType.DMA((5,)),
            pltpu.SemaphoreType.DMA,
            pltpu.SemaphoreType.DMA,
            pltpu.SemaphoreType.REGULAR,
            pltpu.SemaphoreType.REGULAR,
            pltpu.SemaphoreType.DMA,
            pltpu.SemaphoreType.DMA,
            pltpu.SemaphoreType.DMA((PIECES,)),
            pltpu.SemaphoreType.DMA((3,)),
            pltpu.SemaphoreType.DMA((3,)),
        ],
        compiler_params=pltpu.CompilerParams(collective_id=0, has_side_effects=True),
    )(coeffs, snapshots)
    return pl.pallas_call(
        write,
        out_shape=(jax.ShapeDtypeStruct((widths, rows, cols), jnp.float32),
                   jax.ShapeDtypeStruct((widths,), jnp.float32)),
        in_specs=[pl.BlockSpec(memory_space=pl.ANY)] * 2,
        out_specs=[pl.BlockSpec(memory_space=pl.ANY)] * 2,
        scratch_shapes=[pltpu.SemaphoreType.DMA((2,))],
    )(pltpu.with_memory_space_constraint(averages, pltpu.VMEM),
      pltpu.with_memory_space_constraint(norms, pltpu.VMEM))


def solution(mesh):
    split = Mesh(mesh.devices.reshape(mesh.shape["snap"], 2, 4, 4, 2), ("snap",) + PARAM)
    return jax.shard_map(
        on_device,
        mesh=split,
        in_specs=(P("snap", PARAM, None), P(None, "snap")),
        out_specs=(P(None, PARAM, "snap"), P()),
        check_vma=False,
    )
```

```python
import functools

import jax
import jax.numpy as jnp
from jax import lax
from jax.experimental import pallas as pl
from jax.experimental.pallas import tpu as pltpu
from jax.sharding import Mesh
from jax.sharding import PartitionSpec as P

MESH = pl.DeviceIdType.MESH
PARAM = ("zlo", "x", "y", "core")
ROWS = 16
HALF = 8
LEAST = -125.0
SPAN = 251.5
TINY = 1e-37
PIECES = 12
EARLY = ((0, 0, 0, 1), (1, 0, 0, 1), (1, 0, 0, 0))
Z_FAR = (4, 3, -3, 2, -2, 1, -1, 0)
PLANE_FAR = tuple(sorted(((dx, dy) for dx in (-1, 0, 1, 2) for dy in (-1, 0, 1, 2)),
                         key=lambda d: -abs(d[0]) - abs(d[1])))


def encode(value):
    size = jnp.abs(value)
    largest = jnp.max(jnp.max(jnp.max(size, axis=0), axis=0), axis=0, keepdims=True)[None]
    largest = jnp.maximum(largest, TINY)
    inverse = 1.0 / largest
    power = jnp.exp2((size * inverse[:, None]) * SPAN + LEAST)
    return jnp.where(value < 0, -power, power).astype(jnp.bfloat16), largest


def decode(codes, largest):
    code = codes.astype(jnp.float32)
    size = (jnp.log2(jnp.abs(code)) - LEAST) * (largest * (1.0 / SPAN))[:, None]
    return jnp.where(code < 0, -size, size)


def tile_of(i):
    return (i % 2) * 2 + i // 2, 2 * (i % 2) - 1


def kernel(sizes, coeffs_hbm, snap_hbm, avg_out, norm_out,
           avg, norm, coef, stage, kron, sent, sent_max, got, got_max, piece, squares,
           note, seen1, seen2, seen,
           coef_sem, stage_sem, out_sem, norm_sem, relay_sem, all_sem, send_sem, send_max_sem,
           recv_sem, note_send, note_recv):
    widths, snaps, cols, entries = sizes
    halves = widths // HALF
    q = lax.axis_index("snap")
    zlo, x, y, core = (lax.axis_index(a) for a in PARAM)
    line = (q * 2 + zlo) * 2 + core
    plane = x * 4 + y
    z = q * 2 + zlo

    def line_at(dz, to_core):
        z = (q * 2 + zlo + dz + 8) % 8
        return {"snap": z // 2, "zlo": z % 2, "core": to_core}

    def plane_at(dx, dy, to_core):
        return {"x": (x + dx + 4) % 4, "y": (y + dy + 4) % 4, "core": to_core}

    barrier = pltpu.get_barrier_semaphore()

    def load(k, group):
        kind, i = k // 4, k % 4
        tile, way = tile_of(i)
        block = (q + jnp.where(kind == 0, 2, jnp.where(kind == 1, 4 - way, jnp.where(kind == 2, 4 + way, 0)))) % 4
        return pltpu.make_async_copy(
            snap_hbm.at[:, pl.ds(pl.multiple_of(tile * ROWS, ROWS), ROWS),
                        pl.ds(pl.multiple_of(block * cols, cols), cols)],
            stage.at[k], stage_sem.at[group])

    coef_copy = pltpu.make_async_copy(coeffs_hbm, coef, coef_sem)
    coef_copy.start()
    load(0, 0).start()
    near = [line_at(dz, core if same else 1 - core)
            for dz in (-2, 2, -1, 1, 0) for same in (True, False) if dz or not same]
    near += [plane_at(dx, dy, core if same else 1 - core)
             for dx, dy in PLANE_FAR if 0 < abs(dx) + abs(dy) <= 2 for same in (True, False)]
    for peer in near:
        pl.semaphore_signal(barrier, inc=1, device_id=peer, device_id_type=MESH)
    for k in range(1, 16):
        load(k, 1 + (k > 3) + (k > 7) + (k > 11)).start()

    m, n = HALF * ROWS, snaps * ROWS
    across = jnp.where(lax.broadcasted_iota(jnp.int32, (snaps, n), 1) // ROWS
                       == lax.broadcasted_iota(jnp.int32, (snaps, n), 0), 1.0, 0.0).astype(jnp.bfloat16)
    same = jnp.where(lax.broadcasted_iota(jnp.int32, (m, n), 0) % ROWS
                     == lax.broadcasted_iota(jnp.int32, (m, n), 1) % ROWS, 1.0, 0.0).astype(jnp.bfloat16)
    with jax.named_scope("coef_wait"):
        coef_copy.wait()
    part = jnp.broadcast_to(coef[...][:, None, :], (widths, ROWS, snaps)).reshape(widths * ROWS, snaps)
    for p in range(2):
        top = part.astype(jnp.bfloat16)
        part = part - top.astype(jnp.float32)
        spread = jnp.dot(top, across, preferred_element_type=jnp.float32).astype(jnp.bfloat16)
        for h in range(halves):
            kron[pl.ds((h * 2 + p) * m, m), :] = spread[h * m:(h + 1) * m] * same

    def product(k):
        both = jnp.dot(kron[...], stage[k].reshape(n, cols), preferred_element_type=jnp.float32)
        both = both.reshape(halves, 2, HALF, ROWS, cols)
        return both[:, 0] + both[:, 1]

    def copies(k, target):
        peer = {"snap": (q + target + 4) % 4}
        return (
            pltpu.make_async_remote_copy(
                src_ref=sent_max.at[k], dst_ref=got_max.at[k], send_sem=send_max_sem,
                recv_sem=recv_sem.at[k], device_id=peer, device_id_type=MESH),
            pltpu.make_async_remote_copy(
                src_ref=sent.at[k], dst_ref=got.at[k], send_sem=send_sem,
                recv_sem=recv_sem.at[k], device_id=peer, device_id_type=MESH),
        )

    def put(k, value):
        sent[k], sent_max[k] = encode(value)

    def send(k, target):
        for copy in copies(k, target):
            copy.start()

    def receive(k):
        pltpu.make_async_copy(piece, piece, recv_sem.at[k]).wait()
        return decode(got[k], got_max[k]).reshape(widths, ROWS, cols)

    load(0, 0).wait()
    put(0, product(0))
    with jax.named_scope("barrier"):
        pl.semaphore_wait(barrier, len(near))
    send(0, -1)

    def first(k, _):
        tile, way = tile_of(k % 4)
        put(k, product(k))
        send(k, jnp.where(k < 4, way, -way))
        return 0

    def loaded(k, count, group):
        pltpu.make_async_copy(stage.at[pl.ds(k, count)], stage.at[pl.ds(k, count)], stage_sem.at[group]).wait()

    with jax.named_scope("first"):
        loaded(1, 3, 1)
        lax.fori_loop(1, 4, first, 0)
        loaded(4, 4, 2)
        lax.fori_loop(4, 8, first, 0)

    relays = [line_at(-2, core), line_at(2, core), plane_at(2, 0, core), plane_at(0, 2, core)]
    for peer in relays:
        pl.semaphore_signal(relay_sem, inc=1, device_id=peer, device_id_type=MESH)

    def rows_of(i):
        return pl.ds(pl.multiple_of(tile_of(i)[0] * ROWS, ROWS), ROWS)

    def mine(i, _):
        avg[:, rows_of(i), :] = product(12 + i).reshape(widths, ROWS, cols)
        return 0

    loaded(8, 4, 3)
    loaded(12, 4, 4)
    with jax.named_scope("mine"):
        lax.fori_loop(0, 4, mine, 0)

    def forward(i, _):
        tile, way = tile_of(i)
        put(8 + i, product(8 + i) + receive(i).reshape(halves, HALF, ROWS, cols))
        send(8 + i, way)
        return 0

    with jax.named_scope("forward"):
        lax.fori_loop(0, 4, forward, 0)

    pl.semaphore_wait(relay_sem, len(relays))
    for dx, dy in PLANE_FAR[:-1]:
        pl.semaphore_signal(all_sem, inc=1, device_id=plane_at(dx, dy, core), device_id_type=MESH)

    def direct(i, _):
        avg[:, rows_of(i), :] += receive(4 + i)
        return 0

    with jax.named_scope("direct"):
        lax.fori_loop(0, 4, direct, 0)
    squares[...] = jnp.zeros_like(squares)
    with jax.named_scope("relay"):
        pl.semaphore_wait(all_sem, len(PLANE_FAR) - 1)

    def last(i, _):
        value = avg[:, rows_of(i), :] + receive(8 + i)
        avg[:, rows_of(i), :] = value
        square = (value * value).reshape(widths, ROWS // 8, 8, cols)
        squares[...] += jnp.sum(square, axis=1)
        return 0

    with jax.named_scope("last"):
        lax.fori_loop(0, 4, last, 0)
    out = pltpu.make_async_copy(avg, avg_out, out_sem)
    out.start()

    per = jnp.sum(jnp.sum(squares[...], axis=1), axis=1, keepdims=True)
    spot = (lax.broadcasted_iota(jnp.int32, (widths, 128), 0)
            == lax.broadcasted_iota(jnp.int32, (widths, 128), 1))
    value = jnp.sum(jnp.where(spot, per, 0.0), axis=0, keepdims=True)
    note[0] = value
    seen1[line] = value

    def message(step, there, here, peer):
        return pltpu.make_async_remote_copy(
            src_ref=note.at[step % 2], dst_ref=there.at[here], send_sem=note_send.at[step],
            recv_sem=note_recv.at[step], device_id=peer, device_id_type=MESH)

    def wait(sem, count):
        pltpu.make_async_copy(seen.at[pl.ds(0, count)], seen.at[pl.ds(0, count)], sem).wait()

    def line_sum(there, first):
        total = there[first]
        for i in range(1, 16):
            total = total + there[first + i]
        return total

    hub = core == 1
    early = [(z == ez) & (x == ex) & (y == ey) & (core == ec) for ez, ex, ey, ec in EARLY]
    is_early = functools.reduce(jnp.logical_or, early)
    for me, (ez, ex, ey, ec) in zip(early, EARLY):
        @pl.when(jnp.logical_not(me))
        def _():
            message(2, seen, plane * 16 + line,
                    {"snap": ez // 2, "zlo": ez % 2, "x": ex, "y": ey, "core": ec}).start()
    for dz in Z_FAR[:-1]:
        message(0, seen1, line, line_at(dz, 1)).start()

    @pl.when(jnp.logical_not(hub))
    def _():
        message(0, seen1, line, line_at(0, 1)).start()

    with jax.named_scope("drain"):
        pltpu.make_async_copy(sent, sent, send_sem).wait()
        pltpu.make_async_copy(sent_max, sent_max, send_max_sem).wait()

    def spread(skip):
        for dx, dy in PLANE_FAR:
            for to in (0, 1):
                if (dx, dy) == (0, 0) and to == 1:
                    continue
                peer = plane_at(dx, dy, to)
                known = [(z == ez) & (peer["x"] == ex) & (peer["y"] == ey) for ez, ex, ey, ec in EARLY if ec == to]
                if skip and known:
                    @pl.when(jnp.logical_not(functools.reduce(jnp.logical_or, known)))
                    def _():
                        message(1, seen2, plane, peer).start()
                else:
                    message(1, seen2, plane, peer).start()

    planes = sorted({e[0] for e in EARLY})
    early_plane = functools.reduce(jnp.logical_or, [z == ez for ez in planes])

    @pl.when(hub)
    def _():
        with jax.named_scope("norm0"):
            wait(note_recv.at[0], 15)
        total = line_sum(seen1, 0)
        note[1] = total
        seen2[plane] = total

        @pl.when(early_plane)
        def _():
            spread(True)

        @pl.when(jnp.logical_not(early_plane))
        def _():
            spread(False)

    @pl.when(is_early)
    def _():
        seen[plane * 16 + line] = value
        with jax.named_scope("norm2"):
            wait(note_recv.at[2], 255)
        for p in range(16):
            seen2[p] = line_sum(seen, p * 16)

    @pl.when(jnp.logical_not(is_early) & hub)
    def _():
        with jax.named_scope("norm1"):
            wait(note_recv.at[1], 15)

    @pl.when(jnp.logical_not(is_early | hub))
    def _():
        with jax.named_scope("norm1"):
            wait(note_recv.at[1], 16)

    norm[...] = jnp.sqrt(jnp.sum(seen2[...], axis=0) / jnp.float32(entries))[0, :widths]
    norm_copy = pltpu.make_async_copy(norm, norm_out, norm_sem)
    norm_copy.start()

    @pl.when(hub)
    def _():
        wait(note_send.at[0], 7)
        for ez in planes:
            @pl.when(z == ez)
            def _():
                others = [e for e in EARLY if e[0] == ez]
                for me, e in zip(early, EARLY):
                    if e in others and e[3] == 1:
                        @pl.when(me)
                        def _():
                            wait(note_send.at[1], 31 - len(others) + 1)
                hubs = [me for me, e in zip(early, EARLY) if e in others and e[3] == 1]
                if hubs:
                    @pl.when(jnp.logical_not(functools.reduce(jnp.logical_or, hubs)))
                    def _():
                        wait(note_send.at[1], 31 - len(others))
                else:
                    wait(note_send.at[1], 31 - len(others))

        @pl.when(jnp.logical_not(early_plane))
        def _():
            wait(note_send.at[1], 31)

    @pl.when(jnp.logical_not(hub))
    def _():
        wait(note_send.at[0], 8)

    @pl.when(is_early)
    def _():
        if len(EARLY) > 1:
            wait(note_send.at[2], len(EARLY) - 1)

    @pl.when(jnp.logical_not(is_early))
    def _():
        wait(note_send.at[2], len(EARLY))

    out.wait()
    norm_copy.wait()


def write(avg, norm, avg_hbm, norm_hbm, sems):
    large = pltpu.make_async_copy(avg, avg_hbm, sems.at[0])
    small = pltpu.make_async_copy(norm, norm_hbm, sems.at[1])
    large.start()
    small.start()
    small.wait()
    large.wait()


def on_device(snapshots, coeffs):
    widths, snaps = coeffs.shape
    _, rows, all_cols = snapshots.shape
    cols = all_cols // 4
    halves = widths // HALF
    entries = rows * all_cols * 64
    averages, norms = pl.pallas_call(
        functools.partial(kernel, (widths, snaps, cols, entries)),
        out_shape=(pltpu.VMEM((widths, rows, cols), jnp.float32), pltpu.VMEM((widths,), jnp.float32)),
        in_specs=[pl.BlockSpec(memory_space=pl.ANY)] * 2,
        out_specs=[pl.BlockSpec(memory_space=pl.ANY)] * 2,
        scratch_shapes=[
            pltpu.VMEM((widths, rows, cols), jnp.float32),
            pltpu.VMEM((widths,), jnp.float32),
            pltpu.VMEM((widths, snaps), jnp.float32),
            pltpu.VMEM((16, snaps, ROWS, cols), jnp.bfloat16),
            pltpu.VMEM((2 * widths * ROWS, snaps * ROWS), jnp.bfloat16),
            pltpu.VMEM((PIECES, halves, HALF, ROWS, cols), jnp.bfloat16),
            pltpu.VMEM((PIECES, 1, 1, cols), jnp.float32),
            pltpu.VMEM((PIECES, halves, HALF, ROWS, cols), jnp.bfloat16),
            pltpu.VMEM((PIECES, 1, 1, cols), jnp.float32),
            pltpu.VMEM((widths * ROWS // 2 + 1, 1, cols), jnp.float32),
            pltpu.VMEM((widths, 8, cols), jnp.float32),
            pltpu.VMEM((2, 1, 128), jnp.float32),
            pltpu.VMEM((16, 1, 128), jnp.float32),
            pltpu.VMEM((16, 1, 128), jnp.float32),
            pltpu.VMEM((256, 1, 128), jnp.float32),
            pltpu.SemaphoreType.DMA,
            pltpu.SemaphoreType.DMA((5,)),
            pltpu.SemaphoreType.DMA,
            pltpu.SemaphoreType.DMA,
            pltpu.SemaphoreType.REGULAR,
            pltpu.SemaphoreType.REGULAR,
            pltpu.SemaphoreType.DMA,
            pltpu.SemaphoreType.DMA,
            pltpu.SemaphoreType.DMA((PIECES,)),
            pltpu.SemaphoreType.DMA((3,)),
            pltpu.SemaphoreType.DMA((3,)),
        ],
        compiler_params=pltpu.CompilerParams(collective_id=0, has_side_effects=True),
    )(coeffs, snapshots)
    return pl.pallas_call(
        write,
        out_shape=(jax.ShapeDtypeStruct((widths, rows, cols), jnp.float32),
                   jax.ShapeDtypeStruct((widths,), jnp.float32)),
        in_specs=[pl.BlockSpec(memory_space=pl.ANY)] * 2,
        out_specs=[pl.BlockSpec(memory_space=pl.ANY)] * 2,
        scratch_shapes=[pltpu.SemaphoreType.DMA((2,))],
    )(pltpu.with_memory_space_constraint(averages, pltpu.VMEM),
      pltpu.with_memory_space_constraint(norms, pltpu.VMEM))


def solution(mesh):
    split = Mesh(mesh.devices.reshape(mesh.shape["snap"], 2, 4, 4, 2), ("snap",) + PARAM)
    return jax.shard_map(
        on_device,
        mesh=split,
        in_specs=(P("snap", PARAM, None), P(None, "snap")),
        out_specs=(P(None, PARAM, "snap"), P()),
        check_vma=False,
    )
```
